32 devices in a mesh: gx: 2 (over x), gy: 4 (over y, core), gz: 4 (over z).
Axes of the slice: x: 2, y: 2, z: 4, core: 2. Of those that a mesh axis runs over, the one named last changes fastest.
Arguments:
- flow_pops: float32 [19, 16, 32, 512], P(None, 'gx', 'gy', 'gz'), may hold values from 0 to 0.6, as said below
- heat_pops: float32 [7, 16, 32, 512], P(None, 'gx', 'gy', 'gz'), may hold values from -0.2 to 0.2
Outputs:
- flow_out: float32 [19, 16, 32, 512], P(None, 'gx', 'gy', 'gz')
- heat_out: float32 [7, 16, 32, 512], P(None, 'gx', 'gy', 'gz')
- nusselt: float32 [], replicated
The draws below stay inside these ranges and needn't reach their ends.
Inputs may be any that keep to these rules, and one draw needn't show every extreme that they name: `flow_pops`: positive flow populations.
All inputs are finite; a program needn't handle non-finite values.
Results may differ from the reference program's by a relative error of at most 0.0001.
Values sent between devices are 32-bit elements; how exact they have to be, the bound alone decides.
No kernel may reach another device: no remote copies, remote signals or barrier semaphores. Data moves between devices by JAX's collectives and lax.ppermute only.
A program may use at most 64 MiB of HBM per device.

```python
import jax
import jax.numpy as jnp
import numpy as np

STEPS = 3
NX = 16
NY = 32
NZ = 512


FLOW_WEIGHT = np.array([1.0 / 3.0] + [1.0 / 18.0] * 6 + [1.0 / 36.0] * 12)


D3Q7_QUADRATURE = np.array([0.25] + [0.125] * 6)


def draw_flow_pops(key, part):
    weight = jnp.asarray(FLOW_WEIGHT, jnp.float32).reshape(19, 1, 1, 1)
    factor = jax.random.uniform(key, (19, NX, NY, NZ), jnp.float32, 0.8, 1.2)
    return (weight * factor).astype(jnp.float32)


def draw_heat_pops(key, part):
    weight = jnp.asarray(D3Q7_QUADRATURE, jnp.float32).reshape(7, 1, 1, 1)
    noise = jax.random.uniform(jax.random.fold_in(key, 21), (7, NX, NY, NZ), jnp.float32, -0.1, 0.1)
    cell_temp = jax.random.uniform(jax.random.fold_in(key, 23), (1, NX, NY, NZ), jnp.float32, -0.4, 0.4)
    return (weight * (cell_temp + noise)).astype(jnp.float32)


def setup_inputs(seed: int = 0) -> dict:
    splits = jax.random.split(jax.random.key(seed), 3)
    flow_pops = draw_flow_pops(jax.random.fold_in(splits[2], 71), 0)
    heat_pops = draw_heat_pops(jax.random.fold_in(splits[2], 71), 0)
    return dict(flow_pops=flow_pops, heat_pops=heat_pops)


FLOW_SET = np.array([[0, 0, 0], [1, 0, 0], [-1, 0, 0], [0, 1, 0], [0, -1, 0], [0, 0, 1], [0, 0, -1], [1, 1, 0], [-1, -1, 0], [1, -1, 0], [-1, 1, 0], [1, 0, 1], [-1, 0, -1], [1, 0, -1], [-1, 0, 1], [0, 1, 1], [0, -1, -1], [0, 1, -1], [0, -1, 1]])
FLOW_WEIGHT = np.array([1.0 / 3.0] + [1.0 / 18.0] * 6 + [1.0 / 36.0] * 12)
D3Q7_QUADRATURE = np.array([0.25] + [0.125] * 6)
LATTICE = np.concatenate([FLOW_SET, FLOW_SET[:7]], axis=0)
WEIGHTS = np.concatenate([FLOW_WEIGHT, D3Q7_QUADRATURE])
OPPOSITE = np.array([[r for r in range(19) if (FLOW_SET[r] == -FLOW_SET[q]).all()][0] for q in range(19)] + [19 + [r for r in range(7) if (FLOW_SET[r] == -FLOW_SET[q]).all()][0] for q in range(7)])
TAU_FLOW = 0.6
TAU_HEAT = 0.7
GRAVITY_LIFT = 0.01
HOT_WALL = 0.5
COLD_WALL = -0.5
DIFFUSIVITY = (TAU_HEAT - 0.5) / 4.0


def stacked_subarray(values, count):
    return jnp.asarray(values[:count], jnp.float32).reshape(count, 1, 1, 1)


def hydrodynamic_observables(momentum_populations, energy_populations):
    mass_per_site = jnp.sum(momentum_populations, axis=0)
    site_warmth = jnp.sum(energy_populations, axis=0)
    gravity_direction_push = GRAVITY_LIFT * mass_per_site * site_warmth
    speed_xaxis_component = jnp.sum(stacked_subarray(FLOW_SET[:, 0], 19) * momentum_populations, axis=0) / mass_per_site
    speed_yaxis_component = jnp.sum(stacked_subarray(FLOW_SET[:, 1], 19) * momentum_populations, axis=0) / mass_per_site
    speed_zaxis_component = (jnp.sum(stacked_subarray(FLOW_SET[:, 2], 19) * momentum_populations, axis=0) + 0.5 * gravity_direction_push) / mass_per_site
    return mass_per_site, site_warmth, gravity_direction_push, speed_xaxis_component, speed_yaxis_component, speed_zaxis_component


def collide(momentum_populations, energy_populations):
    mass_per_site, site_warmth, gravity_direction_push, speed_xaxis_component, speed_yaxis_component, speed_zaxis_component = hydrodynamic_observables(momentum_populations, energy_populations)
    dir_z = stacked_subarray(FLOW_SET[:, 2], 19)
    projected_onto_link = stacked_subarray(FLOW_SET[:, 0], 19) * speed_xaxis_component + stacked_subarray(FLOW_SET[:, 1], 19) * speed_yaxis_component + dir_z * speed_zaxis_component
    speed_sq = speed_xaxis_component * speed_xaxis_component + speed_yaxis_component * speed_yaxis_component + speed_zaxis_component * speed_zaxis_component
    weight = stacked_subarray(FLOW_WEIGHT, 19)
    equil = weight * mass_per_site * (1.0 + 3.0 * projected_onto_link + 4.5 * projected_onto_link * projected_onto_link - 1.5 * speed_sq)
    source = (1.0 - 0.5 / TAU_FLOW) * weight * (3.0 * (dir_z - speed_zaxis_component) + 9.0 * projected_onto_link * dir_z) * gravity_direction_push
    flow_post = momentum_populations - (momentum_populations - equil) / TAU_FLOW + source
    warmth_rest_distribution = stacked_subarray(D3Q7_QUADRATURE, 7) * site_warmth * (1.0 + 4.0 * projected_onto_link[:7])
    heat_post = energy_populations - (energy_populations - warmth_rest_distribution) / TAU_HEAT
    return jnp.concatenate([flow_post, heat_post], axis=0)


def apply_walls(read, post, is_bottom, is_top):
    result = []
    for member in range(26):
        single = read[member]
        dir_z = int(LATTICE[member, 2])
        if dir_z != 0:
            plane = 0 if dir_z == 1 else single.shape[2] - 1
            flag = is_bottom if dir_z == 1 else is_top
            wall_temp = HOT_WALL if dir_z == 1 else COLD_WALL
            back = post[int(OPPOSITE[member])][:, :, plane]
            if member >= 19:
                back = -back + 2.0 * float(WEIGHTS[member]) * wall_temp
            single = single.at[:, :, plane].set(jnp.where(flag, back, single[:, :, plane]))
        result.append(single)
    return jnp.stack(result)


def local_flux(momentum_populations, energy_populations):
    mass_per_site, site_warmth, gravity_direction_push, speed_xaxis_component, speed_yaxis_component, speed_zaxis_component = hydrodynamic_observables(momentum_populations, energy_populations)
    return jnp.sum(speed_zaxis_component * site_warmth)


def reference(flow_pops, heat_pops):
    momentum_populations, energy_populations = flow_pops, heat_pops
    for period in range(STEPS):
        post = collide(momentum_populations, energy_populations)
        result = []
        for member in range(26):
            single = jnp.roll(post[member], int(LATTICE[member, 0]), 0)
            single = jnp.roll(single, int(LATTICE[member, 1]), 1)
            dir_z = int(LATTICE[member, 2])
            zeros = jnp.zeros(single.shape[:2] + (1,), jnp.float32)
            if dir_z == 1:
                single = jnp.concatenate([zeros, single[:, :, :-1]], axis=2)
            elif dir_z == -1:
                single = jnp.concatenate([single[:, :, 1:], zeros], axis=2)
            result.append(single)
        read = apply_walls(jnp.stack(result), post, True, True)
        momentum_populations, energy_populations = read[:19], read[19:]
    total = local_flux(momentum_populations, energy_populations)
    nusselt = 1.0 + NZ / (DIFFUSIVITY * (HOT_WALL - COLD_WALL)) * total / (NX * NY * NZ)
    return momentum_populations, energy_populations, nusselt.astype(jnp.float32)
```

```python
import functools

import jax
import jax.numpy as jnp
import numpy as np
from jax import lax
from jax.experimental import pallas as pl
from jax.experimental.pallas import tpu as pltpu
from jax.sharding import PartitionSpec as P

STEPS = 3
TAU_FLOW = 0.6
TAU_HEAT = 0.7
GRAVITY_LIFT = 0.01
HOT_WALL = 0.5
COLD_WALL = -0.5
DIFFUSIVITY = (TAU_HEAT - 0.5) / 4.0

FLOW_SET = [
    (0, 0, 0),
    (1, 0, 0),
    (-1, 0, 0),
    (0, 1, 0),
    (0, -1, 0),
    (0, 0, 1),
    (0, 0, -1),
    (1, 1, 0),
    (-1, -1, 0),
    (1, -1, 0),
    (-1, 1, 0),
    (1, 0, 1),
    (-1, 0, -1),
    (1, 0, -1),
    (-1, 0, 1),
    (0, 1, 1),
    (0, -1, -1),
    (0, 1, -1),
    (0, -1, 1),
]
LATTICE = FLOW_SET + FLOW_SET[:7]
COUNT = len(LATTICE)
NFLOW = len(FLOW_SET)
OPPOSITE = [
    (0 if q < NFLOW else NFLOW) + FLOW_SET.index(tuple(-c for c in LATTICE[q])) for q in range(COUNT)
]
HEAT_WEIGHT = [0.25] + [0.125] * 6
MOVING = {
    (axis, sign): [q for q in range(COUNT) if LATTICE[q][axis] == sign]
    for axis in range(3)
    for sign in (1, -1)
}
FACE = len(MOVING[0, 1])
SLOT = 8


def lanes_of(shape):
    return lax.broadcasted_iota(jnp.int32, shape, 1)


def rows_of(shape):
    return lax.broadcasted_iota(jnp.int32, shape, 0)


def roll(tile, amount, axis):
    size = tile.shape[axis]
    amount = amount % size
    return tile if amount == 0 else pltpu.roll(tile, amount, axis)


def pack(tiles):
    lane = lanes_of(tiles[0].shape)
    packed = None
    for slot, tile in enumerate(tiles):
        tile = roll(tile, STEPS + SLOT * slot, 1)
        packed = tile if packed is None else jnp.where(lane >= SLOT * slot, tile, packed)
    return packed


def unpack(packed, slot):
    return roll(packed, -(STEPS + SLOT * slot), 1)


def moments(f):
    rho = functools.reduce(lambda a, b: a + b, f[:NFLOW])
    temp = functools.reduce(lambda a, b: a + b, f[NFLOW:])
    diff = {q: f[q] - f[q + 1] for q in range(1, NFLOW, 2)}
    flux = []
    for axis in range(3):
        total = None
        for q in range(1, NFLOW, 2):
            c = LATTICE[q][axis]
            if c:
                assert total is not None or c == 1
                total = diff[q] if total is None else total + diff[q] if c == 1 else total - diff[q]
        flux.append(total)
    push = GRAVITY_LIFT * rho * temp
    inverse = 1.0 / rho
    return rho, temp, push, flux[0] * inverse, flux[1] * inverse, (flux[2] + 0.5 * push) * inverse


def collide(f):
    rho, temp, push, ux, uy, uz = moments(f)
    u = (ux, uy, uz)
    keep = 1.0 - 1.0 / TAU_FLOW
    scale = rho * (1.0 / TAU_FLOW / 36.0)
    source = push * ((1.0 - 0.5 / TAU_FLOW) / 36.0)
    base = scale * (1.0 - 1.5 * (ux * ux + uy * uy + uz * uz)) - 3.0 * source * uz
    linear, square = 3.0 * scale, 4.5 * scale
    push1, push2 = 3.0 * source, 9.0 * source
    out = [None] * COUNT
    out[0] = keep * f[0] + 12.0 * base
    for q in range(1, NFLOW, 2):
        c = LATTICE[q]
        along = None
        for axis in range(3):
            if c[axis]:
                along = u[axis] if along is None else along + u[axis] if c[axis] == 1 else along - u[axis]
        inner = square * along
        odd = linear * along
        if c[2] == 1:
            inner, odd = inner + push2, odd + push1
        elif c[2] == -1:
            inner, odd = inner - push2, odd - push1
        even = base + inner * along
        if q < 7:
            even, odd = 2.0 * even, 2.0 * odd
        out[q] = keep * f[q] + (even + odd)
        out[q + 1] = keep * f[q + 1] + (even - odd)
    keep = 1.0 - 1.0 / TAU_HEAT
    out[NFLOW] = keep * f[NFLOW] + (HEAT_WEIGHT[0] / TAU_HEAT) * temp
    rest = (HEAT_WEIGHT[1] / TAU_HEAT) * temp
    for axis in range(3):
        q = NFLOW + 1 + 2 * axis
        drift = 4.0 * rest * u[axis]
        out[q] = keep * f[q] + (rest + drift)
        out[q + 1] = keep * f[q + 1] + (rest - drift)
    return out


def send(outs, up, down, odd):
    if len(outs) == 1:
        for j, tile in enumerate(up + down):
            outs[0][j] = tile
    else:
        for j in range(len(up)):
            outs[0][j] = jnp.where(odd, down[j], up[j])
            outs[1][j] = jnp.where(odd, up[j], down[j])


def received(ins, odd, count):
    if len(ins) == 1:
        return (lambda j: ins[0][j]), (lambda j: ins[0][count + j])
    low = lambda j: jnp.where(odd, ins[0][j], ins[1][j])
    high = lambda j: jnp.where(odd, ins[1][j], ins[0][j])
    return low, high


def swap(buffers, axis, size, periodic):
    if size == 1:
        return list(buffers)
    first = [(i, i + 1) for i in range(0, size - 1, 2)]
    second = [(i, i + 1) for i in range(1, size - 1, 2)] + ([(size - 1, 0)] if periodic else [])
    both = lambda pairs: [p for a, b in pairs for p in ((a, b), (b, a))]
    if len(buffers) == 1:
        return [lax.ppermute(buffers[0], axis, both(first))]
    return [lax.ppermute(b, axis, both(pairs)) for b, pairs in zip(buffers, (first, second))]


def face_x(post, halo, extent):
    up = [post(q, extent - 1) for q in MOVING[0, 1]]
    down = [post(q, 0) for q in MOVING[0, -1]]
    up.append(pack([halo(q, extent - 1) for q in MOVING[0, 1]]))
    down.append(pack([halo(q, 0) for q in MOVING[0, -1]]))
    return up, down


def call(kernel, ins, outs, flops, scratch=()):
    vmem = pl.BlockSpec(memory_space=pltpu.VMEM)
    smem = pl.BlockSpec(memory_space=pltpu.SMEM)
    return pl.pallas_call(
        kernel,
        out_shape=[jax.ShapeDtypeStruct(s, jnp.float32) for s in outs],
        in_specs=[smem] + [vmem] * (len(ins) - 1),
        out_specs=[vmem] * len(outs),
        scratch_shapes=[pltpu.VMEM(s, jnp.float32) for s in scratch],
        compiler_params=pltpu.CompilerParams(vmem_limit_bytes=12 * 2**20),
        cost_estimate=pl.CostEstimate(flops=flops, bytes_accessed=flops // 8, transcendentals=0),
    )(*ins)


def per_device(sizes, flow, heat):
    X, Y, Z = flow.shape[1:]
    assert Z >= 2 * STEPS and Z % SLOT == 0
    slots = Z // SLOT
    ztiles = -(-COUNT * X // slots)
    nx, ny, nz = (sizes[a] for a in ("gx", "gy", "gz"))
    assert all(n == 1 or n % 2 == 0 for n in (nx, ny, nz))
    tile = (Y, Z)
    bx = 1 if nx <= 2 else 2
    by = 1 if ny <= 2 else 2
    xshape = (2 * (FACE + 1) // bx, Y, Z)
    yshape = (2 * (FACE + 1) // by, X, Z)
    big = (COUNT, X, Y, Z)
    ix, iy, iz = (lax.axis_index(a) for a in ("gx", "gy", "gz"))
    info = jnp.stack([ix % 2, iy % 2, iz % 2, iz == 0, iz == nz - 1]).astype(jnp.int32)
    work = COUNT * X * Y * Z * 10

    def whole(flow_ref, heat_ref):
        return lambda q, x: flow_ref[q, x] if q < NFLOW else heat_ref[q - NFLOW, x]

    def pack_z(info_ref, flow_ref, heat_ref, out_ref):
        get = whole(flow_ref, heat_ref)
        entries = [(q, x) for q in range(COUNT) for x in range(X)]
        for t in range(ztiles):
            out_ref[t] = pack([get(q, x) for q, x in entries[t * slots : (t + 1) * slots]])

    def first_main(info_ref, flow_ref, heat_ref, post_ref):
        get = whole(flow_ref, heat_ref)
        for x in range(X):
            for q, value in enumerate(collide([get(q, x) for q in range(COUNT)])):
                post_ref[q, x] = value

    def first_halo(info_ref, za_ref, zb_ref, post_ref, halo_ref, *x_refs):
        merged = x_refs[-1]
        odd_z = info_ref[2] == 1
        inner = lanes_of(tile) % SLOT < STEPS
        for t in range(ztiles):
            a, b = za_ref[t], zb_ref[t]
            low, high = jnp.where(odd_z, a, b), jnp.where(odd_z, b, a)
            merged[t] = jnp.where(inner, low, high)
        for x in range(X):
            f = []
            for q in range(COUNT):
                t, slot = divmod(q * X + x, slots)
                f.append(unpack(merged[t], slot))
            for q, value in enumerate(collide(f)):
                halo_ref[q, x] = value
        up, down = face_x(lambda q, x: post_ref[q, x], lambda q, x: halo_ref[q, x], X)
        send(x_refs[:-1], up, down, info_ref[0] == 1)

    def pack_y(info_ref, post_ref, halo_ref, *refs):
        x_refs, y_refs = refs[:bx], refs[bx:]
        x_low, x_high = received(x_refs, info_ref[0] == 1, FACE + 1)
        sub = rows_of((X, Z))

        def rows(q, row):
            main, halo = post_ref[q, :, row, :], halo_ref[q, :, row, :]
            cx = LATTICE[q][0]
            if cx:
                source, members = (x_low, MOVING[0, 1]) if cx == 1 else (x_high, MOVING[0, -1])
                j = members.index(q)
                edge = sub == (0 if cx == 1 else X - 1)
                at_main = source(j)[row : row + 1, :]
                at_halo = unpack(source(FACE)[row : row + 1, :], j)
                main = jnp.where(edge, at_main, roll(main, cx, 0))
                halo = jnp.where(edge, at_halo, roll(halo, cx, 0))
            return main, halo

        ways = []
        for sign, row in ((1, Y - 1), (-1, 0)):
            pairs = [rows(q, row) for q in MOVING[1, sign]]
            ways.append([m for m, _ in pairs] + [pack([h for _, h in pairs])])
        send(y_refs, ways[0], ways[1], info_ref[1] == 1)

    def stream(info_ref, post_ref, halo_ref, x_refs, y_refs, yh_ref, use):
        x_low, x_high = received(x_refs, info_ref[0] == 1, FACE + 1)
        y_low, y_high = received(y_refs, info_ref[1] == 1, FACE + 1)
        lane, sub = lanes_of(tile), rows_of(tile)
        first, last = lane == 0, lane == Z - 1
        at_bottom = first & (info_ref[3] == 1)
        at_top = last & (info_ref[4] == 1)
        for j in range(FACE):
            yh_ref[j] = unpack(y_low(FACE), j)
            yh_ref[FACE + j] = unpack(y_high(FACE), j)
            yh_ref[2 * FACE + j] = y_low(j)
            yh_ref[3 * FACE + j] = y_high(j)
        for x in range(X):
            mains, halos = [], []
            for q in range(COUNT):
                cx, cy, cz = LATTICE[q]
                if 0 <= x - cx < X:
                    main, halo = post_ref[q, x - cx], halo_ref[q, x - cx]
                else:
                    source, members = (x_low, MOVING[0, 1]) if cx == 1 else (x_high, MOVING[0, -1])
                    j = members.index(q)
                    main, halo = source(j), unpack(source(FACE), j)
                if cy:
                    j = MOVING[1, cy].index(q) + (0 if cy == 1 else FACE)
                    edge = sub == (0 if cy == 1 else Y - 1)
                    main = jnp.where(edge, yh_ref[2 * FACE + j, x : x + 1, :], roll(main, cy, 0))
                    halo = jnp.where(edge, yh_ref[j, x : x + 1, :], roll(halo, cy, 0))
                if cz:
                    edge, wall = (first, at_bottom) if cz == 1 else (last, at_top)
                    main, halo = roll(main, cz, 1), roll(halo, cz, 1)
                    main, halo = jnp.where(edge, halo, main), jnp.where(edge, main, halo)
                    back = post_ref[OPPOSITE[q], x]
                    if q >= NFLOW:
                        at_wall = HOT_WALL if cz == 1 else COLD_WALL
                        back = 2.0 * HEAT_WEIGHT[q - NFLOW] * at_wall - back
                    main = jnp.where(wall, back, main)
                mains.append(main)
                halos.append(halo)
            use(x, mains, halos)

    def middle(info_ref, post_ref, halo_ref, *refs):
        x_refs, y_refs, refs = refs[:bx], refs[bx : bx + by], refs[bx + by :]
        new_ref, new_halo_ref, xo_refs, yh_ref = refs[0], refs[1], refs[2:-1], refs[-1]

        def use(x, mains, halos):
            for q, value in enumerate(halos):
                new_halo_ref[q, x] = value
            for q, value in enumerate(collide(mains)):
                new_ref[q, x] = value
            for q, value in enumerate(collide([new_halo_ref[q, x] for q in range(COUNT)])):
                new_halo_ref[q, x] = value

        stream(info_ref, post_ref, halo_ref, x_refs, y_refs, yh_ref, use)
        up, down = face_x(lambda q, x: new_ref[q, x], lambda q, x: new_halo_ref[q, x], X)
        send(xo_refs, up, down, info_ref[0] == 1)

    devices = nx * ny * nz

    def final(info_ref, post_ref, halo_ref, *refs):
        x_refs, y_refs, refs = refs[:bx], refs[bx : bx + by], refs[bx + by :]
        flow_ref, heat_ref, part_ref, yh_ref = refs
        total = [jnp.zeros(tile, jnp.float32)]

        def use(x, mains, halos):
            for q, value in enumerate(mains):
                if q < NFLOW:
                    flow_ref[q, x] = value
                else:
                    heat_ref[q - NFLOW, x] = value
            _, temp, _, _, _, uz = moments(mains)
            total[0] = total[0] + uz * temp

        stream(info_ref, post_ref, halo_ref, x_refs, y_refs, yh_ref, use)
        part = jnp.sum(total[0], axis=0, keepdims=True)
        part_ref[...] = jnp.broadcast_to(part[None], part_ref.shape)

    (zpack,) = call(pack_z, (info, flow, heat), [(ztiles, Y, Z)], work)
    za, zb = swap([zpack, zpack], "gz", nz, False)
    (post,) = call(first_main, (info, flow, heat), [big], 20 * work)
    post_halo, *xs = call(
        first_halo, (info, za, zb, post), [big] + [xshape] * bx, 20 * work, [(ztiles, Y, Z)]
    )
    for step in range(STEPS):
        xs = swap(xs, "gx", nx, True)
        ys = call(pack_y, (info, post, post_halo, *xs), [yshape] * by, work)
        ys = swap(ys, "gy", ny, True)
        ins = (info, post, post_halo, *xs, *ys)
        scratch = [(4 * FACE, X, Z)]
        if step < STEPS - 1:
            post, post_halo, *xs = call(middle, ins, [big, big] + [xshape] * bx, 20 * work, scratch)
        else:
            flow, heat, parts = call(
                final, ins, [flow.shape, heat.shape, (devices, 1, Z)], 20 * work, scratch
            )
    parts = lax.all_to_all(parts, ("gx", "gy", "gz"), 0, 0, tiled=True)
    cells = X * Y * Z * devices
    factor = Z * nz / (DIFFUSIVITY * (HOT_WALL - COLD_WALL)) / cells
    nusselt = 1.0 + factor * jnp.sum(parts)
    return flow, heat, nusselt


def solution(mesh):
    placed = P(None, "gx", "gy", "gz")
    return jax.shard_map(
        functools.partial(per_device, dict(mesh.shape)),
        mesh=mesh,
        in_specs=(placed, placed),
        out_specs=(placed, placed, P()),
        check_vma=False,
    )
```

```python
import functools

import jax
import jax.numpy as jnp
import numpy as np
from jax import lax
from jax.experimental import pallas as pl
from jax.experimental.pallas import tpu as pltpu
from jax.sharding import PartitionSpec as P

STEPS = 3
TAU_FLOW = 0.6
TAU_HEAT = 0.7
GRAVITY_LIFT = 0.01
HOT_WALL = 0.5
COLD_WALL = -0.5
DIFFUSIVITY = (TAU_HEAT - 0.5) / 4.0

FLOW_SET = [
    (0, 0, 0),
    (1, 0, 0),
    (-1, 0, 0),
    (0, 1, 0),
    (0, -1, 0),
    (0, 0, 1),
    (0, 0, -1),
    (1, 1, 0),
    (-1, -1, 0),
    (1, -1, 0),
    (-1, 1, 0),
    (1, 0, 1),
    (-1, 0, -1),
    (1, 0, -1),
    (-1, 0, 1),
    (0, 1, 1),
    (0, -1, -1),
    (0, 1, -1),
    (0, -1, 1),
]
LATTICE = FLOW_SET + FLOW_SET[:7]
COUNT = len(LATTICE)
NFLOW = len(FLOW_SET)
OPPOSITE = [
    (0 if q < NFLOW else NFLOW) + FLOW_SET.index(tuple(-c for c in LATTICE[q])) for q in range(COUNT)
]
HEAT_WEIGHT = [0.25] + [0.125] * 6
MOVING = {
    (axis, sign): [q for q in range(COUNT) if LATTICE[q][axis] == sign]
    for axis in range(3)
    for sign in (1, -1)
}
FACE = len(MOVING[0, 1])
SLOT = 8


def lanes_of(shape):
    return lax.broadcasted_iota(jnp.int32, shape, 1)


def rows_of(shape):
    return lax.broadcasted_iota(jnp.int32, shape, 0)


def roll(tile, amount, axis):
    size = tile.shape[axis]
    amount = amount % size
    return tile if amount == 0 else pltpu.roll(tile, amount, axis)


def spread(row, shape):
    return jnp.broadcast_to(row, shape)


def total_of(values):
    return functools.reduce(lambda a, b: a + b, values)


def moments(f):
    rho = functools.reduce(lambda a, b: a + b, f[:NFLOW])
    temp = functools.reduce(lambda a, b: a + b, f[NFLOW:])
    diff = {q: f[q] - f[q + 1] for q in range(1, NFLOW, 2)}
    flux = []
    for axis in range(3):
        total = None
        for q in range(1, NFLOW, 2):
            c = LATTICE[q][axis]
            if c:
                assert total is not None or c == 1
                total = diff[q] if total is None else total + diff[q] if c == 1 else total - diff[q]
        flux.append(total)
    push = GRAVITY_LIFT * rho * temp
    inverse = 1.0 / rho
    return rho, temp, push, flux[0] * inverse, flux[1] * inverse, (flux[2] + 0.5 * push) * inverse


def collide(f):
    rho, temp, push, ux, uy, uz = moments(f)
    u = (ux, uy, uz)
    keep = 1.0 - 1.0 / TAU_FLOW
    scale = rho * (1.0 / TAU_FLOW / 36.0)
    source = push * ((1.0 - 0.5 / TAU_FLOW) / 36.0)
    base = scale * (1.0 - 1.5 * (ux * ux + uy * uy + uz * uz)) - 3.0 * source * uz
    linear, square = 3.0 * scale, 4.5 * scale
    push1, push2 = 3.0 * source, 9.0 * source
    out = [None] * COUNT
    out[0] = keep * f[0] + 12.0 * base
    for q in range(1, NFLOW, 2):
        c = LATTICE[q]
        along = None
        for axis in range(3):
            if c[axis]:
                along = u[axis] if along is None else along + u[axis] if c[axis] == 1 else along - u[axis]
        inner = square * along
        odd = linear * along
        if c[2] == 1:
            inner, odd = inner + push2, odd + push1
        elif c[2] == -1:
            inner, odd = inner - push2, odd - push1
        even = base + inner * along
        if q < 7:
            even, odd = 2.0 * even, 2.0 * odd
        out[q] = keep * f[q] + (even + odd)
        out[q + 1] = keep * f[q + 1] + (even - odd)
    keep = 1.0 - 1.0 / TAU_HEAT
    out[NFLOW] = keep * f[NFLOW] + (HEAT_WEIGHT[0] / TAU_HEAT) * temp
    rest = (HEAT_WEIGHT[1] / TAU_HEAT) * temp
    for axis in range(3):
        q = NFLOW + 1 + 2 * axis
        drift = 4.0 * rest * u[axis]
        out[q] = keep * f[q] + (rest + drift)
        out[q + 1] = keep * f[q + 1] + (rest - drift)
    return out


def parity(axis):
    return lax.axis_index(axis) % 2 == 1


def send(outs, up, down, odd):
    if len(outs) == 1:
        for j, tile in enumerate(up + down):
            outs[0][j] = tile
    else:
        for j in range(len(up)):
            outs[0][j] = jnp.where(odd, down[j], up[j])
            outs[1][j] = jnp.where(odd, up[j], down[j])


def received(ins, odd, count):
    if len(ins) == 1:
        return {1: lambda j: ins[0][j], -1: lambda j: ins[0][count + j]}
    return {
        1: lambda j: jnp.where(odd, ins[0][j], ins[1][j]),
        -1: lambda j: jnp.where(odd, ins[1][j], ins[0][j]),
    }


def swap_pairs(size, periodic):
    first = [(i, i + 1) for i in range(0, size - 1, 2)]
    second = [(i, i + 1) for i in range(1, size - 1, 2)] + ([(size - 1, 0)] if periodic else [])
    return [[p for a, b in pairs for p in ((a, b), (b, a))] for pairs in (first, second)]


def swap(buffers, axis, size, periodic=True):
    if size == 1:
        return list(buffers)
    routes = swap_pairs(size, periodic)
    return [lax.ppermute(b, axis, route) for b, route in zip(buffers, routes)]


def swap_corners(buffers, nx, ny):
    routes = [[(0, 0)], []] if ny == 1 else swap_pairs(ny, True)
    moved = {}
    for way in (1, -1):
        if way == -1 and nx <= 2:
            moved[way] = moved[1]
            continue
        moved[way] = [
            lax.ppermute(
                b,
                ("gx", "gy"),
                [(x * ny + i, (x + way) % nx * ny + j) for x in range(nx) for i, j in route],
            )
            for b, route in zip(buffers, routes)
        ]
    return moved


def call(kernel, ins, outs, flops, scratch=(), in_space=pltpu.VMEM, out_space=None, sems=0):
    out_space = [pltpu.VMEM] * len(outs) if out_space is None else out_space
    return pl.pallas_call(
        kernel,
        out_shape=[jax.ShapeDtypeStruct(s, jnp.float32) for s in outs],
        in_specs=[pl.BlockSpec(memory_space=in_space)] * len(ins),
        out_specs=[pl.BlockSpec(memory_space=s) for s in out_space],
        scratch_shapes=[pltpu.VMEM(s, jnp.float32) for s in scratch]
        + ([pltpu.SemaphoreType.DMA((sems,))] if sems else []),
        compiler_params=pltpu.CompilerParams(vmem_limit_bytes=12 * 2**20),
        cost_estimate=pl.CostEstimate(flops=flops, bytes_accessed=flops // 8, transcendentals=0),
    )(*ins)


def per_device(sizes, flow, heat):
    X, Y, Z = flow.shape[1:]
    slots = Z // SLOT
    nx, ny, nz = (sizes[a] for a in ("gx", "gy", "gz"))
    assert all(n == 1 or n % 2 == 0 for n in (nx, ny, nz))
    assert 2 * STEPS <= SLOT and STEPS <= Z and Z % SLOT == 0
    assert slots % X == 0 and FACE <= X and FACE <= slots and Y >= 4
    share = slots // X
    ztiles = -(-COUNT // share)
    tile = (Y, Z)
    bx = 1 if nx <= 2 else 2
    by = 1 if ny <= 2 else 2
    ways = 1 if nx <= 2 else 2
    big, ring = (COUNT, X, Y, Z), (COUNT, Y, Z)
    message_shapes = (
        [(2 * (FACE + 1) // bx, Y, Z)] * bx
        + [(2 * (FACE + 1) // by, X, Z)] * by
        + [(2 // by, Y, Z)] * by
    )
    work = COUNT * X * Y * Z * 10
    start = (X - 1) * SLOT

    def whole(flow_ref, heat_ref):
        return lambda q, x: flow_ref[q, x] if q < NFLOW else heat_ref[q - NFLOW, x]

    def pack_z(flow_ref, heat_ref, pack_ref):
        get = whole(flow_ref, heat_ref)
        lane = lanes_of(tile)
        for t in range(ztiles):
            packed = None
            for k, q in enumerate(range(t * share, min((t + 1) * share, COUNT))):
                for x in range(X):
                    slot = k * X + x
                    moved = roll(get(q, x), STEPS + SLOT * slot, 1)
                    packed = moved if slot == 0 else jnp.where(lane >= SLOT * slot, moved, packed)
            pack_ref[t] = packed

    def first_main(flow_ref, heat_ref, post_ref):
        get = whole(flow_ref, heat_ref)
        for x in range(X):
            for q, value in enumerate(collide([get(q, x) for q in range(COUNT)])):
                post_ref[q, x] = value

    def emit(post_ref, ring_ref, outs):
        x_outs, outs = outs[:bx], outs[bx:]
        y_outs, edge_outs = outs[:by], outs[by:]
        lane, sub, subx = lanes_of(tile), rows_of(tile), rows_of((X, Z))
        sent = []
        for sign, x, at in ((1, X - 1, start), (-1, 0, 0)):
            packed = None
            for j, q in enumerate(MOVING[0, sign]):
                moved = roll(ring_ref[q], SLOT * j - at, 1)
                packed = moved if j == 0 else jnp.where(lane >= SLOT * j, moved, packed)
            sent.append([post_ref[q, x] for q in MOVING[0, sign]] + [packed])
        send(x_outs, sent[0], sent[1], parity("gx"))
        odd = parity("gy")
        rows, edges = [], []
        for sign, y in ((1, Y - 1), (-1, 0)):
            packed = None
            for j, q in enumerate(MOVING[1, sign]):
                row = spread(ring_ref[q, y : y + 1, :], (X, Z))
                packed = row if j == 0 else jnp.where(subx == j, row, packed)
            rows.append([post_ref[q, :, y, :] for q in MOVING[1, sign]] + [packed])
            edge = None
            for k, cx in enumerate((1, -1)):
                q = LATTICE.index((cx, sign, 0))
                x = X - 1 if cx == 1 else 0
                main = spread(post_ref[q, x, y : y + 1, :], tile)
                halo = spread(ring_ref[q, y : y + 1, :], tile)
                edge = main if k == 0 else jnp.where(sub == k, main, edge)
                edge = jnp.where(sub == k + 2, halo, edge)
            edges.append([edge])
        send(y_outs, rows[0], rows[1], odd)
        send(edge_outs, edges[0], edges[1], odd)

    def first_halo(za_ref, zb_ref, post_ref, ring_ref, *outs):
        odd = parity("gz")
        inner = lanes_of(tile) % SLOT < STEPS
        f = []
        for t in range(ztiles):
            a, b = za_ref[t], zb_ref[t]
            merged = jnp.where(inner, jnp.where(odd, a, b), jnp.where(odd, b, a))
            for k, q in enumerate(range(t * share, min((t + 1) * share, COUNT))):
                f.append(roll(merged, -k * X * SLOT, 1))
        for q, value in enumerate(collide(f)):
            ring_ref[q] = value
        emit(post_ref, ring_ref, outs)

    def stream(post_ref, ring_ref, refs, yrow, state, state_ring, done):
        x_refs, refs = refs[:bx], refs[bx:]
        y_refs, refs = refs[:by], refs[by:]
        odd_y = parity("gy")
        from_x = received(x_refs, parity("gx"), FACE + 1)
        from_y = received(y_refs, odd_y, FACE + 1)
        from_edge = {
            (way, sign): received(refs[i * by : (i + 1) * by], odd_y, 1)[sign](0)
            for way, i in ((1, 0), (-1, ways - 1))
            for sign in (1, -1)
        }
        lane, sub = lanes_of(tile), rows_of(tile)
        ends = {1: lane == 0, -1: lane == Z - 1}
        on_wall = {
            1: ends[1] & (lax.axis_index("gz") == 0),
            -1: ends[-1] & (lax.axis_index("gz") == nz - 1),
        }
        borders = {1: sub == 0, -1: sub == Y - 1}
        x_slot = {1: lane < SLOT, -1: lane >= start}
        x_ring = {sign: from_x[sign](FACE) for sign in (1, -1)}
        y_ring = {sign: from_y[sign](FACE) for sign in (1, -1)}
        for sign in (1, -1):
            for j in range(FACE):
                yrow[j if sign == 1 else FACE + j] = from_y[sign](j)

        def ring_of(q):
            cx, cy, _ = LATTICE[q]
            t = ring_ref[q]
            if cx:
                j = MOVING[0, cx].index(q)
                edge = roll(x_ring[cx], (0 if cx == 1 else start) - SLOT * j, 1)
                t = jnp.where(x_slot[cx], edge, roll(t, SLOT * cx, 1))
            if cy:
                j = MOVING[1, cy].index(q)
                row = spread(y_ring[cy][j : j + 1, :], tile)
                if cx:
                    k = 2 if cx == 1 else 3
                    corner = roll(spread(from_edge[cx, cy][k : k + 1, :], tile), -start * cx, 1)
                    row = jnp.where(x_slot[cx], corner, roll(row, SLOT * cx, 1))
                t = jnp.where(borders[cy], row, roll(t, cy, 0))
            return t

        for q in range(COUNT):
            cx, cy, cz = LATTICE[q]
            around = ring_of(q) if cz or state_ring is not None else None
            grown = roll(around, cz, 1) if cz and state_ring is not None else around
            for x in range(X):
                inside = 0 <= x - cx < X
                t = post_ref[q, x - cx] if inside else from_x[cx](MOVING[0, cx].index(q))
                if cy:
                    j = MOVING[1, cy].index(q) + (0 if cy == 1 else FACE)
                    if inside:
                        row = yrow[j, x - cx : x - cx + 1, :]
                    else:
                        k = 0 if cx == 1 else 1
                        row = from_edge[cx, cy][k : k + 1, :]
                    t = jnp.where(borders[cy], spread(row, tile), roll(t, cy, 0))
                if cz:
                    near = SLOT * x + (STEPS - 1 if cz == 1 else STEPS)
                    far = SLOT * x + (STEPS if cz == 1 else STEPS - 1)
                    end = 0 if cz == 1 else Z - 1
                    if state_ring is not None:
                        grown = jnp.where(lane == far, roll(t, far - end + cz, 1), grown)
                    back = post_ref[OPPOSITE[q], x]
                    if q >= NFLOW:
                        wall = HOT_WALL if cz == 1 else COLD_WALL
                        back = 2.0 * HEAT_WEIGHT[q - NFLOW] * wall - back
                    t = jnp.where(ends[cz], roll(around, end - near, 1), roll(t, cz, 1))
                    t = jnp.where(on_wall[cz], back, t)
                state[q, x] = t
            if state_ring is not None:
                state_ring[q] = grown
            done(q)

    def middle(post_ref, ring_ref, *refs):
        given = bx + by * (1 + ways)
        ins, new_ref, new_ring_ref = refs[:given], refs[given], refs[given + 1]
        outs, yrow = refs[given + 2 : -1], refs[-1]
        stream(post_ref, ring_ref, ins, yrow, new_ref, new_ring_ref, lambda q: None)
        for x in range(X):
            for q, value in enumerate(collide([new_ref[q, x] for q in range(COUNT)])):
                new_ref[q, x] = value
        for q, value in enumerate(collide([new_ring_ref[q] for q in range(COUNT)])):
            new_ring_ref[q] = value
        emit(new_ref, new_ring_ref, outs)

    devices = nx * ny * nz

    def final(post_ref, ring_ref, *refs):
        given = bx + by * (1 + ways)
        ins, (flow_ref, heat_ref, part_ref, yrow, state, sems) = refs[:given], refs[given:]
        copies = [
            pltpu.make_async_copy(
                state.at[q], flow_ref.at[q] if q < NFLOW else heat_ref.at[q - NFLOW], sems.at[q]
            )
            for q in range(COUNT)
        ]
        stream(post_ref, ring_ref, ins, yrow, state, None, lambda q: copies[q].start())
        parts = []
        for x in range(X):
            _, temp, _, _, _, uz = moments([state[q, x] for q in range(COUNT)])
            parts.append(uz * temp)
        part = jnp.sum(total_of(parts), axis=0, keepdims=True)
        part_ref[...] = jnp.broadcast_to(part[None], part_ref.shape)
        for copy in copies:
            copy.wait()

    cells = X * Y * Z * devices
    factor = Z * nz / (DIFFUSIVITY * (HOT_WALL - COLD_WALL)) / cells

    def finish(parts_ref, out_ref):
        part = jnp.sum(parts_ref[...], axis=0)
        out_ref[...] = 1.0 + factor * jnp.sum(part, axis=1, keepdims=True)

    def exchange(messages):
        xs, messages = messages[:bx], messages[bx:]
        ys, edges = messages[:by], messages[by:]
        xs = swap(xs, "gx", nx)
        ys = swap(ys, "gy", ny)
        moved = swap_corners(edges, nx, ny)
        edges = moved[1] + (moved[-1] if ways == 2 else [])
        return [*xs, *ys, *edges]

    (zpack,) = call(pack_z, (flow, heat), [(ztiles, Y, Z)], work)
    za, zb = swap([zpack, zpack], "gz", nz, False)
    (post,) = call(first_main, (flow, heat), [big], 20 * work)
    around, *messages = call(first_halo, (za, zb, post), [ring] + message_shapes, 2 * work)
    scratch = [(2 * FACE, X, Z)]
    for step in range(STEPS - 1):
        ins = (post, around, *exchange(messages))
        post, around, *messages = call(middle, ins, [big, ring] + message_shapes, 20 * work, scratch)
    flow, heat, parts = call(
        final,
        (post, around, *exchange(messages)),
        [flow.shape, heat.shape, (devices, 1, Z)],
        20 * work,
        scratch + [big],
        out_space=[pltpu.HBM, pltpu.HBM, pltpu.VMEM],
        sems=COUNT,
    )
    parts = lax.all_to_all(parts, ("gx", "gy", "gz"), 0, 0, tiled=True)
    (nusselt,) = call(finish, (parts,), [(1, 1)], work)
    return flow, heat, nusselt.reshape(())


def solution(mesh):
    placed = P(None, "gx", "gy", "gz")
    return jax.shard_map(
        functools.partial(per_device, dict(mesh.shape)),
        mesh=mesh,
        in_specs=(placed, placed),
        out_specs=(placed, placed, P()),
        check_vma=False,
    )
```

```python
import functools

import jax
import jax.numpy as jnp
import numpy as np
from jax import lax
from jax.experimental import pallas as pl
from jax.experimental.pallas import tpu as pltpu
from jax.sharding import PartitionSpec as P

STEPS = 3
TAU_FLOW = 0.6
TAU_HEAT = 0.7
GRAVITY_LIFT = 0.01
HOT_WALL = 0.5
COLD_WALL = -0.5
DIFFUSIVITY = (TAU_HEAT - 0.5) / 4.0

FLOW_SET = [
    (0, 0, 0),
    (1, 0, 0),
    (-1, 0, 0),
    (0, 1, 0),
    (0, -1, 0),
    (0, 0, 1),
    (0, 0, -1),
    (1, 1, 0),
    (-1, -1, 0),
    (1, -1, 0),
    (-1, 1, 0),
    (1, 0, 1),
    (-1, 0, -1),
    (1, 0, -1),
    (-1, 0, 1),
    (0, 1, 1),
    (0, -1, -1),
    (0, 1, -1),
    (0, -1, 1),
]
LATTICE = FLOW_SET + FLOW_SET[:7]
COUNT = len(LATTICE)
NFLOW = len(FLOW_SET)
OPPOSITE = [
    (0 if q < NFLOW else NFLOW) + FLOW_SET.index(tuple(-c for c in LATTICE[q])) for q in range(COUNT)
]
HEAT_WEIGHT = [0.25] + [0.125] * 6
MOVING = {
    (axis, sign): [q for q in range(COUNT) if LATTICE[q][axis] == sign]
    for axis in range(3)
    for sign in (1, -1)
}
FACE = len(MOVING[0, 1])
SLOT = 8


def lanes_of(shape):
    return lax.broadcasted_iota(jnp.int32, shape, 1)


def rows_of(shape):
    return lax.broadcasted_iota(jnp.int32, shape, 0)


def roll(tile, amount, axis):
    size = tile.shape[axis]
    amount = amount % size
    return tile if amount == 0 else pltpu.roll(tile, amount, axis)


def spread(row, shape):
    return jnp.broadcast_to(row, shape)


def total_of(values):
    return functools.reduce(lambda a, b: a + b, values)


def moments(f):
    rho = functools.reduce(lambda a, b: a + b, f[:NFLOW])
    temp = functools.reduce(lambda a, b: a + b, f[NFLOW:])
    diff = {q: f[q] - f[q + 1] for q in range(1, NFLOW, 2)}
    flux = []
    for axis in range(3):
        total = None
        for q in range(1, NFLOW, 2):
            c = LATTICE[q][axis]
            if c:
                assert total is not None or c == 1
                total = diff[q] if total is None else total + diff[q] if c == 1 else total - diff[q]
        flux.append(total)
    push = GRAVITY_LIFT * rho * temp
    inverse = 1.0 / rho
    return rho, temp, push, flux[0] * inverse, flux[1] * inverse, (flux[2] + 0.5 * push) * inverse


def collide(f):
    rho, temp, push, ux, uy, uz = moments(f)
    u = (ux, uy, uz)
    keep = 1.0 - 1.0 / TAU_FLOW
    scale = rho * (1.0 / TAU_FLOW / 36.0)
    source = push * ((1.0 - 0.5 / TAU_FLOW) / 36.0)
    base = scale * (1.0 - 1.5 * (ux * ux + uy * uy + uz * uz)) - 3.0 * source * uz
    linear, square = 3.0 * scale, 4.5 * scale
    push1, push2 = 3.0 * source, 9.0 * source
    out = [None] * COUNT
    out[0] = keep * f[0] + 12.0 * base
    for q in range(1, NFLOW, 2):
        c = LATTICE[q]
        along = None
        for axis in range(3):
            if c[axis]:
                along = u[axis] if along is None else along + u[axis] if c[axis] == 1 else along - u[axis]
        inner = square * along
        odd = linear * along
        if c[2] == 1:
            inner, odd = inner + push2, odd + push1
        elif c[2] == -1:
            inner, odd = inner - push2, odd - push1
        even = base + inner * along
        if q < 7:
            even, odd = 2.0 * even, 2.0 * odd
        out[q] = keep * f[q] + (even + odd)
        out[q + 1] = keep * f[q + 1] + (even - odd)
    keep = 1.0 - 1.0 / TAU_HEAT
    out[NFLOW] = keep * f[NFLOW] + (HEAT_WEIGHT[0] / TAU_HEAT) * temp
    rest = (HEAT_WEIGHT[1] / TAU_HEAT) * temp
    for axis in range(3):
        q = NFLOW + 1 + 2 * axis
        drift = 4.0 * rest * u[axis]
        out[q] = keep * f[q] + (rest + drift)
        out[q + 1] = keep * f[q + 1] + (rest - drift)
    return out


def parity(axis):
    return lax.axis_index(axis) % 2 == 1


def send(outs, up, down, odd, at, count):
    for j in range(len(up)):
        if len(outs) == 1:
            outs[0][at + j] = up[j]
            outs[0][count + at + j] = down[j]
        else:
            outs[0][at + j] = jnp.where(odd, down[j], up[j])
            outs[1][at + j] = jnp.where(odd, up[j], down[j])


def send_rows(outs, up, down, odd, count):
    height = outs[0].shape[1]
    for i in range(len(up)):
        t, r = divmod(i, height)
        if len(outs) == 1:
            outs[0][t, r : r + 1, :] = up[i]
            outs[0][count + t, r : r + 1, :] = down[i]
        else:
            outs[0][t, r : r + 1, :] = jnp.where(odd, down[i], up[i])
            outs[1][t, r : r + 1, :] = jnp.where(odd, up[i], down[i])


def received(ins, odd, count):
    if len(ins) == 1:
        return {1: lambda j: ins[0][j], -1: lambda j: ins[0][count + j]}
    return {
        1: lambda j: jnp.where(odd, ins[0][j], ins[1][j]),
        -1: lambda j: jnp.where(odd, ins[1][j], ins[0][j]),
    }


def swap_pairs(size, periodic=True):
    if size == 1:
        return [[(0, 0)], [(0, 0)]]
    first = [(i, i + 1) for i in range(0, size - 1, 2)]
    second = [(i, i + 1) for i in range(1, size - 1, 2)] + ([(size - 1, 0)] if periodic else [])
    return [[p for a, b in pairs for p in ((a, b), (b, a))] for pairs in (first, second)]


def swap(buffers, axis, size, periodic=True):
    if size == 1:
        return list(buffers)
    return [lax.ppermute(b, axis, route) for b, route in zip(buffers, swap_pairs(size, periodic))]


def swap_corners(buffers, nx, ny):
    moved = {}
    for way in (1, -1) if nx > 2 else (1,):
        moved[way] = []
        for b, along_y in zip(buffers, swap_pairs(ny)):
            route = [(x * ny + y, (x + way) % nx * ny + to) for x in range(nx) for y, to in along_y]
            moved[way].append(lax.ppermute(b, ("gx", "gy"), route))
    return [b for way in moved for b in moved[way]]


def call(kernel, ins, outs, flops, scratch=(), in_space=None, out_space=None, sems=0, alias=None):
    in_space = [pltpu.VMEM] * len(ins) if in_space is None else in_space
    out_space = [pltpu.VMEM] * len(outs) if out_space is None else out_space
    return pl.pallas_call(
        kernel,
        out_shape=[jax.ShapeDtypeStruct(s, jnp.float32) for s in outs],
        in_specs=[pl.BlockSpec(memory_space=s) for s in in_space],
        out_specs=[pl.BlockSpec(memory_space=s) for s in out_space],
        scratch_shapes=[pltpu.VMEM(s, jnp.float32) for s in scratch]
        + ([pltpu.SemaphoreType.DMA((sems,))] if sems else []),
        input_output_aliases=alias or {},
        compiler_params=pltpu.CompilerParams(vmem_limit_bytes=12 * 2**20),
        cost_estimate=pl.CostEstimate(flops=flops, bytes_accessed=flops // 8, transcendentals=0),
    )(*ins)


def plane_reader(refs, X):
    if len(refs) == 1:
        return lambda q, x: refs[0][q, x]
    return lambda q, x: refs[0][q, x - 1] if 0 < x < X - 1 else refs[1][q, 0 if x == 0 else 1]


def per_device(sizes, flow, heat):
    X, Y, Z = flow.shape[1:]
    slots = Z // SLOT
    half = slots // 2
    nx, ny, nz = (sizes[a] for a in ("gx", "gy", "gz"))
    assert all(n == 1 or n % 2 == 0 for n in (nx, ny, nz))
    assert STEPS > 1 and 2 * STEPS <= SLOT and 2 * STEPS <= Y and STEPS <= Z and Z % SLOT == 0
    assert slots % X == 0 and FACE <= half and X > 2 and 4 * (STEPS - 1) <= Y
    share = slots // X
    ztiles = -(-COUNT // share)
    groups = -(-COUNT // X)
    tile = (Y, Z)
    bx = 1 if nx <= 2 else 2
    by = 1 if ny <= 2 else 2
    big, ring = (COUNT, X, Y, Z), (groups * X, Y, Z)
    inner_big, outer_big = (COUNT, X - 2, Y, Z), (COUNT, 2, Y, Z)
    inner_xs, outer_xs = range(1, X - 1), (0, X - 1)

    def needed(q, j, sign):
        _, cy, cz = LATTICE[q]
        return j == 1 or cy == sign or (j < STEPS and (cy == 0 or cz != 0))

    rows = {
        sign: [(q, j) for j in range(1, STEPS + 1) for q in range(COUNT) if needed(q, j, sign)]
        for sign in (1, -1)
    }
    corner_rows = {
        sign: [
            (way, q, j)
            for way in (1, -1)
            for j in range(1, STEPS + 1)
            for q in MOVING[0, way]
            if needed(q, j, sign)
        ]
        for sign in (1, -1)
    }
    cut = len(corner_rows[1])
    ctiles = -(-(cut + 2 * STEPS) // Y)
    row_of = {1: lambda j: Y - j, -1: lambda j: j - 1}
    ymain = len(rows[1])
    ytiles = ymain + (STEPS - 1) * groups + 1
    ways = 1 if nx <= 2 else 2
    x_first, x_later = FACE + 1, FACE + FACE // 2 + 1
    yshape = [(2 * ytiles // by, X, Z)] * by
    cshape = [(2 * ctiles // by, Y, Z)] * by
    xshape = lambda n: [(2 * n // bx, Y, Z)] * bx
    climbing = MOVING[2, 1] + MOVING[2, -1]
    work = COUNT * X * Y * Z * 10

    def load(flow_ref, heat_ref, raw_ref, pack_ref, sems):
        bounds = [0, NFLOW // 2 + 1, NFLOW, COUNT]
        copies = [
            pltpu.make_async_copy(
                flow_ref.at[a:b] if a < NFLOW else heat_ref.at[a - NFLOW : b - NFLOW],
                raw_ref.at[a:b],
                sems.at[i],
            )
            for i, (a, b) in enumerate(zip(bounds, bounds[1:]))
        ]
        for copy in copies:
            copy.start()
        lane = lanes_of(tile)
        for t in range(ztiles):
            packed = None
            for k, q in enumerate(range(t * share, min((t + 1) * share, COUNT))):
                if q in bounds:
                    copies[bounds.index(q)].wait()
                for x in range(X):
                    slot = k * X + x
                    moved = roll(raw_ref[q, x], STEPS + SLOT * slot, 1)
                    packed = moved if slot == 0 else jnp.where(lane >= SLOT * slot, moved, packed)
            pack_ref[t] = packed

    def first_main(raw_ref, post_ref, *y_refs):
        for x in range(X):
            for q, value in enumerate(collide([raw_ref[q, x] for q in range(COUNT)])):
                post_ref[q, x] = value
        send(y_refs, *(y_rows(post_ref, sign) for sign in (1, -1)), parity("gy"), 0, ytiles)

    def y_rows(post_ref, sign):
        return [post_ref[q, :, row_of[sign](j), :] for q, j in rows[sign]]

    def pack_rings(rings, sign):
        lane, packed = lanes_of(tile), None
        for i, ring_ref in enumerate(rings):
            for j, q in enumerate(MOVING[0, sign]):
                to = i * half + j
                moved = roll(ring_ref[q], SLOT * (to - (X - 1 if sign == 1 else 0)), 1)
                packed = moved if packed is None else jnp.where(lane >= SLOT * to, moved, packed)
        return packed

    def first_halo(za_ref, zb_ref, post_ref, *refs):
        y_before, refs = refs[:by], refs[by:]
        ring_ref, x_outs, refs = refs[0], refs[1 : 1 + bx], refs[1 + bx :]
        y_outs, corner_outs, packed_ref = refs[:by], refs[by : 2 * by], refs[2 * by]
        odd = parity("gz")
        inside = lanes_of(tile) % SLOT < STEPS
        f = []
        for t in range(ztiles):
            a, b = za_ref[t], zb_ref[t]
            merged = jnp.where(inside, jnp.where(odd, a, b), jnp.where(odd, b, a))
            for k, q in enumerate(range(t * share, min((t + 1) * share, COUNT))):
                f.append(roll(merged, -k * X * SLOT, 1))
        for q, value in enumerate(collide(f)):
            ring_ref[q] = value
        for q in range(COUNT, groups * X):
            ring_ref[q] = jnp.zeros(tile, jnp.float32)
        faces = []
        for i, (way, x) in enumerate(((1, X - 1), (-1, 0))):
            packed = pack_rings([ring_ref], way)
            packed_ref[i] = packed
            faces.append([post_ref[q, x] for q in MOVING[0, way]] + [packed])
        send(x_outs, faces[0], faces[1], parity("gx"), 0, x_first)
        odd = parity("gy")
        faces, corners = [], []
        for sign in (1, -1):
            at = row_of[sign]
            tiles = [
                ring_ref[g * X : (g + 1) * X, at(j), :] for j in range(1, STEPS) for g in range(groups)
            ]
            last = None
            for k, q in enumerate(MOVING[1, sign]):
                row = spread(ring_ref[q, at(STEPS) : at(STEPS) + 1, :], (X, Z))
                last = row if k == 0 else jnp.where(rows_of((X, Z)) == k, row, last)
            faces.append(tiles + [last])
            corners.append(
                [
                    post_ref[q, X - 1 if way == 1 else 0, at(j) : at(j) + 1, :]
                    for way, q, j in corner_rows[sign]
                ]
                + [packed_ref[i, at(j) : at(j) + 1, :] for i in (0, 1) for j in range(1, STEPS + 1)]
            )
        send(y_outs, faces[0], faces[1], odd, ymain, ytiles)
        send_rows(corner_outs, corners[0], corners[1], odd, ctiles)

    def edges_first(x_refs, corner_refs, edge_ref):
        odd_y = parity("gy")
        from_x = received(x_refs, parity("gx"), x_first)
        for i, way in enumerate((1, -1)):
            refs = corner_refs[:by] if way == 1 or ways == 1 else corner_refs[by:]
            for sign in (1, -1):
                at = row_of[sign]
                entries = [
                    (i * FACE + MOVING[0, way].index(q), j, n)
                    for n, (w, q, j) in enumerate(corner_rows[sign])
                    if w == way
                ] + [(2 * FACE + i, j, cut + i * STEPS + j - 1) for j in range(1, STEPS + 1)]
                for to, j, n in entries:
                    t, r = divmod(n, Y)
                    if by == 1:
                        row = refs[0][t if sign == 1 else ctiles + t, r : r + 1, :]
                    else:
                        a, b = refs[0][t, r : r + 1, :], refs[1][t, r : r + 1, :]
                        row = jnp.where(odd_y, a, b) if sign == 1 else jnp.where(odd_y, b, a)
                    edge_ref[to, at(j) : at(j) + 1, :] = row
        ring_tiles = {
            1: (from_x[1](FACE), edge_ref[2 * FACE]),
            -1: (from_x[-1](FACE), edge_ref[2 * FACE + 1]),
        }

        def around(cx, j):
            return edge_ref[j if cx == 1 else FACE + j]

        def ring_edge(cx, j, i):
            return roll(ring_tiles[cx][i], SLOT * ((0 if cx == 1 else X - 1) - j), 1)

        return (lambda cx, j: from_x[cx](j)), around, ring_edge

    def edges_later(x_refs):
        from_x = received(x_refs, parity("gx"), x_later)
        ring_tiles = {cx: from_x[cx](x_later - 1) for cx in (1, -1)}

        def around(cx, j):
            t = from_x[cx](FACE + j // 2)
            return roll(t, Y // 2, 0) if j % 2 else t

        def ring_edge(cx, j, i):
            return roll(ring_tiles[cx], SLOT * ((0 if cx == 1 else X - 1) - i * half - j), 1)

        return (lambda cx, j: from_x[cx](j)), around, ring_edge

    def send_later(outs, main, side, rings):
        sub = rows_of(tile)
        near = (sub < Y // 4) | (sub >= Y - Y // 4)
        faces = []
        for sign, x in ((1, X - 1), (-1, 0)):
            moving = MOVING[0, sign]
            pairs = [
                jnp.where(near, side(a, x), roll(side(b, x), Y // 2, 0))
                for a, b in zip(moving[::2], moving[1::2])
            ]
            faces.append([main(q, x) for q in moving] + pairs + [pack_rings(rings, sign)])
        send(outs, faces[0], faces[1], parity("gx"), 0, x_later)

    def stream(main, side, rings, edges, xs, put, put_ring, grown_refs=None, last=False, done=None):
        lane, sub = lanes_of(tile), rows_of(tile)
        ends = {1: lane == 0, -1: lane == Z - 1}
        on_wall = {
            1: ends[1] & (lax.axis_index("gz") == 0),
            -1: ends[-1] & (lax.axis_index("gz") == nz - 1),
        }
        borders = {1: sub == 0, -1: sub == Y - 1}
        x_slot = {1: lane < SLOT, -1: lane >= SLOT * (X - 1)}
        edge_main, edge_side, edge_ring = edges if edges else (None, None, None)

        def along_y(t, u, cy):
            if not cy:
                return t, u
            t, u = roll(t, cy, 0), roll(u, cy, 0)
            return jnp.where(borders[cy], u, t), jnp.where(borders[cy], t, u)

        for q in range(COUNT):
            cx, cy, cz = LATTICE[q]
            around = grown = None
            if cz or put_ring:
                around = [rings[0][q], rings[1][q]]
                if cx:
                    around = [roll(t, SLOT * cx, 1) for t in around]
                    if edges:
                        j = MOVING[0, cx].index(q)
                        around = [
                            jnp.where(x_slot[cx], edge_ring(cx, j, i), t) for i, t in enumerate(around)
                        ]
                around = along_y(*around, cy)
                grown = around
            if cz and put_ring:
                grown = [roll(t, cz, 1) for t in around]
                if grown_refs:
                    far = STEPS if cz == 1 else STEPS - 1
                    other = (lane % SLOT == far) & (lane >= SLOT) & (lane < SLOT * (X - 1))
                    i = climbing.index(q)
                    grown = [jnp.where(other, ref[i], t) for ref, t in zip(grown_refs, grown)]
            for x in xs:
                if 0 <= x - cx < X:
                    t, u = main(q, x - cx), side(q, x - cx) if cy or not last else None
                else:
                    j = MOVING[0, cx].index(q)
                    t, u = edge_main(cx, j), edge_side(cx, j) if cy or not last else None
                t, u = along_y(t, u, cy)
                if cz:
                    near = SLOT * x + (STEPS - 1 if cz == 1 else STEPS)
                    far = SLOT * x + (STEPS if cz == 1 else STEPS - 1)
                    end = 0 if cz == 1 else Z - 1
                    if put_ring:
                        grown = [
                            jnp.where(lane == far, roll(v, far - end + cz, 1), g)
                            for v, g in zip((t, u), grown)
                        ]

                    def along_z(v, beside, plane):
                        back = plane(OPPOSITE[q], x)
                        if q >= NFLOW:
                            wall = HOT_WALL if cz == 1 else COLD_WALL
                            back = 2.0 * HEAT_WEIGHT[q - NFLOW] * wall - back
                        v = jnp.where(ends[cz], roll(beside, end - near, 1), roll(v, cz, 1))
                        return jnp.where(on_wall[cz], back, v)

                    t = along_z(t, around[0], main)
                    u = None if last else along_z(u, around[1], side)
                put(q, x, t, u)
            if put_ring:
                put_ring(q, grown)
            if done:
                done(q)

    def collide_in(ref, planes):
        for x in planes:
            for q, value in enumerate(collide([ref[q, x] for q in range(COUNT)])):
                ref[q, x] = value

    def collide_ring(ref):
        for q, value in enumerate(collide([ref[q] for q in range(COUNT)])):
            ref[q] = value

    def putter(main_ref, side_ref, at):
        def put(q, x, t, u):
            main_ref[q, at(x)] = t
            if side_ref is not None:
                side_ref[q, at(x)] = u

        return put

    def ring_putter(refs):
        def put_ring(q, values):
            for ref, value in zip(refs, values):
                ref[q] = value

        return put_ring

    def first_step(post_ref, ring_ref, *refs):
        x_refs, refs = refs[:bx], refs[bx:]
        y_refs, refs = refs[:by], refs[by:]
        corner_refs, refs = refs[: by * ways], refs[by * ways :]
        new_ref, new_side, new_ring, new_ring_side = refs[:4]
        outs, side_ref, ring_side, edge_ref = refs[4:-3], refs[-3], refs[-2], refs[-1]
        from_y = received(y_refs, parity("gy"), ytiles)
        for sign in (1, -1):
            at = row_of[sign]
            for i, (q, j) in enumerate(rows[sign]):
                side_ref[q, :, at(j), :] = from_y[sign](i)
            i = ymain
            for j in range(1, STEPS):
                for g in range(groups):
                    ring_side[g * X : (g + 1) * X, at(j), :] = from_y[sign](i)
                    i += 1
            last = from_y[sign](i)
            for k, q in enumerate(MOVING[1, sign]):
                ring_side[q, at(STEPS) : at(STEPS) + 1, :] = last[k : k + 1, :]
        main, side = plane_reader([post_ref], X), plane_reader([side_ref], X)
        edges = edges_first(x_refs, corner_refs, edge_ref)
        put = putter(new_ref, new_side, lambda x: x)
        put_ring = ring_putter((new_ring, new_ring_side))
        stream(main, side, (ring_ref, ring_side), edges, range(X), put, put_ring)
        for ref in (new_ref, new_side):
            collide_in(ref, range(X))
        for ref in (new_ring, new_ring_side):
            collide_ring(ref)
        main, side = plane_reader([new_ref], X), plane_reader([new_side], X)
        send_later(outs, main, side, (new_ring, new_ring_side))

    def state_of(refs, parts):
        main = plane_reader(refs[:parts], X)
        side = plane_reader(refs[parts : 2 * parts], X)
        return main, side, refs[2 * parts : 2 * parts + 2], refs[2 * parts + 2 :]

    def inner_step(parts, *refs):
        main, side, rings, refs = state_of(refs, parts)
        new_ref, new_side, grown_ref, grown_side = refs

        def put_ring(q, values):
            if q in climbing:
                grown_ref[climbing.index(q)] = values[0]
                grown_side[climbing.index(q)] = values[1]

        put = putter(new_ref, new_side, lambda x: x - 1)
        stream(main, side, rings, None, inner_xs, put, put_ring)
        for ref in (new_ref, new_side):
            collide_in(ref, range(X - 2))

    def outer_step(parts, *refs):
        main, side, rings, refs = state_of(refs, parts)
        x_refs, refs = refs[:bx], refs[bx:]
        grown_refs, refs = refs[:2], refs[2:]
        new_ref, new_side, new_ring, new_ring_side = refs[:4]
        outs = refs[4:]
        put = putter(new_ref, new_side, lambda x: 0 if x == 0 else 1)
        put_ring = ring_putter((new_ring, new_ring_side))
        edges = edges_later(x_refs)
        stream(main, side, rings, edges, outer_xs, put, put_ring, grown_refs)
        for ref in (new_ref, new_side):
            collide_in(ref, range(2))
        for ref in (new_ring, new_ring_side):
            collide_ring(ref)
        at = lambda ref: lambda q, x: ref[q, 0 if x == 0 else 1]
        send_later(outs, at(new_ref), at(new_side), (new_ring, new_ring_side))

    def flux(ref, planes):
        parts = []
        for x in planes:
            _, temp, _, _, _, uz = moments([ref[q, x] for q in range(COUNT)])
            parts.append(uz * temp)
        return total_of(parts)

    def copies_of(source, flow_ref, heat_ref, where, sems):
        return [
            pltpu.make_async_copy(source.at[a:b], ref.at[:, where], sem)
            for ref, a, b, sem in zip((flow_ref, heat_ref), (0, NFLOW), (NFLOW, COUNT), sems)
        ]

    def inner_last(parts, *refs):
        main, side, rings, refs = state_of(refs, parts)
        flow_ref, heat_ref, part_ref, new_ref, sems = refs
        put = putter(new_ref, None, lambda x: x - 1)
        stream(main, side, rings, None, inner_xs, put, None, last=True)
        copies = copies_of(new_ref, flow_ref, heat_ref, slice(1, X - 1), [sems.at[0], sems.at[1]])
        for copy in copies:
            copy.start()
        part_ref[...] = flux(new_ref, range(X - 2))
        for copy in copies:
            copy.wait()

    devices = nx * ny * nz

    def outer_last(parts, *refs):
        main, side, rings, refs = state_of(refs, parts)
        x_refs, (inner_part, new_ref, part_ref) = refs[:bx], refs[bx:]
        put = putter(new_ref, None, lambda x: 0 if x == 0 else 1)
        stream(main, side, rings, edges_later(x_refs), outer_xs, put, None, last=True)
        part = jnp.sum(flux(new_ref, range(2)) + inner_part[...], axis=0, keepdims=True)
        part_ref[...] = jnp.broadcast_to(part[None], part_ref.shape)

    cells = X * Y * Z * devices
    factor = Z * nz / (DIFFUSIVITY * (HOT_WALL - COLD_WALL)) / cells

    def finish(parts_ref, outer_ref, flow_in, heat_in, flow_ref, heat_ref, out_ref, number, sems):
        copies = []
        for i, x in enumerate(outer_xs):
            copies += copies_of(
                outer_ref.at[:, i], flow_ref, heat_ref, x, [sems.at[2 * i], sems.at[2 * i + 1]]
            )
        for copy in copies:
            copy.start()
        part = jnp.sum(parts_ref[...], axis=0)
        number[...] = 1.0 + factor * jnp.sum(part, axis=1, keepdims=True)
        copies.append(pltpu.make_async_copy(number, out_ref, sems.at[4]))
        copies[-1].start()
        for copy in copies:
            copy.wait()

    flow, heat = (pltpu.with_memory_space_constraint(a, pltpu.HBM) for a in (flow, heat))
    raw, zpack = call(
        load, (flow, heat), [big, (ztiles, Y, Z)], work, in_space=[pltpu.HBM] * 2, sems=3
    )
    za, zb = swap([zpack, zpack], "gz", nz, False)
    post, *ys = call(first_main, (raw,), [big] + yshape, 20 * work)
    around, *buffers = call(
        first_halo,
        (za, zb, post, *ys),
        [ring] + xshape(x_first) + yshape + cshape,
        2 * work,
        [(2, Y, Z)],
        alias={3 + i: 1 + bx + i for i in range(by)},
    )
    xs, ys, corners = buffers[:bx], buffers[bx : bx + by], buffers[bx + by :]
    moved = [*swap(xs, "gx", nx), *swap(ys, "gy", ny), *swap_corners(corners, nx, ny)]
    main, side, ring_main, ring_side, *xs = call(
        first_step,
        (post, around, *moved),
        [big, big, ring, ring] + xshape(x_later),
        40 * work,
        [big, ring, (2 * FACE + 2, Y, Z)],
    )
    main, side = [main], [side]
    grown_shape = (len(climbing), Y, Z)
    for _ in range(STEPS - 2):
        state = (*main, *side, ring_main, ring_side)
        xs = swap(xs, "gx", nx)
        inner, inner_side, *grown = call(
            functools.partial(inner_step, len(main)),
            state,
            [inner_big, inner_big, grown_shape, grown_shape],
            40 * work,
        )
        outer, outer_side, ring_main, ring_side, *xs = call(
            functools.partial(outer_step, len(main)),
            (*state, *xs, *grown),
            [outer_big, outer_big, ring, ring] + xshape(x_later),
            10 * work,
        )
        main, side = [inner, outer], [inner_side, outer_side]
    state = (*main, *side, ring_main, ring_side)
    xs = swap(xs, "gx", nx)
    flow, heat, inner_part = call(
        functools.partial(inner_last, len(main)),
        state,
        [flow.shape, heat.shape, tile],
        40 * work,
        [inner_big],
        out_space=[pltpu.HBM, pltpu.HBM, pltpu.VMEM],
        sems=2,
    )
    outer, parts = call(
        functools.partial(outer_last, len(main)),
        (*state, *xs, inner_part),
        [outer_big, (devices, 1, Z)],
        10 * work,
    )
    parts = lax.all_to_all(parts, ("gx", "gy", "gz"), 0, 0, tiled=True)
    flow, heat, nusselt = call(
        finish,
        (parts, outer, flow, heat),
        [flow.shape, heat.shape, (1, 1)],
        work,
        [(1, 1)],
        in_space=[pltpu.VMEM, pltpu.VMEM, pltpu.HBM, pltpu.HBM],
        out_space=[pltpu.HBM, pltpu.HBM, pltpu.HBM],
        sems=5,
        alias={2: 0, 3: 1},
    )
    return flow, heat, nusselt.reshape(())


def solution(mesh):
    placed = P(None, "gx", "gy", "gz")
    return jax.shard_map(
        functools.partial(per_device, dict(mesh.shape)),
        mesh=mesh,
        in_specs=(placed, placed),
        out_specs=(placed, placed, P()),
        check_vma=False,
    )
```
